256 devices in a mesh: band: 128 (over z, y, x), ch: 2 (over core).
Axes of the slice: x: 4, y: 4, z: 8, core: 2. Of those that a mesh axis runs over, the one named last changes fastest.
Arguments:
- grid_field: bfloat16 [100, 2097152], P(None, 'band'), may hold values from -6 to 6
- band_points: int32 [128], P('band'), may hold values from 8192 to 16384
- block_ids: int32 [128, 16], P('band'), may hold values from 0 to 4095, as said below
- block_count: int32 [128], P('band'), may hold values from 8 to 16
- block_weight: bfloat16 [128, 16, 256, 512], P('band'), may hold values from 0 to 0.039794922
- embed_weight: bfloat16 [100, 1024], P(None, 'ch'), may hold values from -0.3125 to 0.3125
- edge_src: int32 [655360], P('band'), may hold values from 0 to 32767, as said below
- edge_dst: int32 [655360], P('band'), may hold values from 0 to 32767, as said below
- edge_in_weight: bfloat16 [2, 1024, 1024], P(None, None, 'ch'), may hold values from -0.1875 to 0.1875
- edge_out_weight: bfloat16 [1024, 1024], P('ch'), may hold values from -0.0625 to 0.0625
- node_in_weight: bfloat16 [2, 1024, 1024], P(None, None, 'ch'), may hold values from -0.125 to 0.125
- node_out_weight: bfloat16 [1024, 1024], P('ch'), may hold values from -0.1875 to 0.1875
Outputs:
- node_state: bfloat16 [32768, 1024], P('band', 'ch')
The draws below stay inside these ranges and needn't reach their ends.
Inputs may be any that keep to these rules, and one draw needn't show every extreme that they name: For band b, block_ids[b, k] * 512 lies from max(b * 16384 - 16384 // 2, 0) to min((b + 1) * 16384 + 16384 // 2, 2097152) - 512; both ends are named by every band; ids may repeat. `edge_src`: edge e belongs to band b = e // 5120; its source node lies in bands b - 1 to b + 1 of the mesh. `edge_dst`: edge e ends at a node of its band b = e // 5120.
All inputs are finite; a program needn't handle non-finite values.
Results may differ from the reference program's by a relative error of at most 0.015.
Values may be sent and summed in bfloat16 or wider, within the bound.
No kernel may reach another device: no remote copies, remote signals or barrier semaphores. Data moves between devices by JAX's collectives and lax.ppermute only.
A program may use at most 64 MiB of HBM per device.

```python
import jax
import jax.numpy as jnp
from jax import lax

CIN = 100
H = 1024
PTS_DEV = 16384
NODE_DEV = 256
E_DEV = 5120
PBLK = 512
K = 16
POINTS = 2097152
NODES = 32768
EDGES = 655360
N_BAND = 128


def draw_block_ids(key, part):
    sub_count = PTS_DEV // PBLK
    band_index = jnp.arange(N_BAND, dtype=jnp.int32)[:, None]
    lowest = jnp.maximum(band_index * sub_count - sub_count // 2, 0)
    highest = jnp.minimum((band_index + 1) * sub_count + sub_count // 2, N_BAND * sub_count)
    raw_bits = jax.random.randint(jax.random.fold_in(key, 11), (N_BAND, K), 0, 1 << 30)
    picked = lowest + raw_bits % (highest - lowest)
    slot_index = jnp.arange(K, dtype=jnp.int32)[None, :]
    picked = jnp.where(slot_index == 0, lowest, picked)
    picked = jnp.where(slot_index == 1, highest - 1, picked)
    return picked.astype(jnp.int32)


def draw_edge_src(key, part):
    edge_index = jnp.arange(EDGES, dtype=jnp.int32)
    band_index = edge_index // E_DEV
    lowest = jnp.maximum(band_index - 1, 0) * NODE_DEV
    highest = jnp.minimum(band_index + 2, N_BAND) * NODE_DEV
    return jax.random.randint(jax.random.fold_in(key, 21), (EDGES,), lowest, highest).astype(jnp.int32)


def draw_edge_dst(key, part):
    edge_index = jnp.arange(EDGES, dtype=jnp.int32)
    band_index = edge_index // E_DEV
    offset = jax.random.randint(jax.random.fold_in(key, 31), (EDGES,), 0, NODE_DEV)
    return (band_index * NODE_DEV + offset).astype(jnp.int32)


def set_ends(drawn, rng, low, high):
    spot = [jax.random.randint(jax.random.fold_in(rng, axis), (), 0, length) for axis, length in enumerate(drawn.shape)]
    longest = drawn.shape.index(max(drawn.shape))
    neighbour = spot[:longest] + [(spot[longest] + 1) % drawn.shape[longest]] + spot[longest + 1:]
    return drawn.at[tuple(spot)].set(low).at[tuple(neighbour)].set(high)


def block_levels(stream_key, extent, shards, low, top_value):
    level, own = 1.0, jax.random.fold_in(stream_key, 6)
    for dim, parts in shards:
        draws = jnp.exp(jax.random.uniform(jax.random.fold_in(own, dim), (parts,), jnp.float32, low / len(shards), top_value / len(shards)))
        level = level * jnp.repeat(draws, extent[dim] // parts).reshape([-1 if axis == dim else 1 for axis in range(len(extent))])
    return level


def bell_draw(stream_key, dims, scale, most, split=(), kind=jnp.bfloat16):
    entries = jax.random.normal(stream_key, dims, jnp.float32) * scale
    if len(split) > 0:
        entries = block_levels(stream_key, dims, split, -0.22, 0.18) * entries
    return jnp.clip(entries, min=-most, max=most).astype(kind)


def setup_inputs(seed: int = 0) -> dict:
    streams_of = jax.random.split(jax.random.key(seed), 13)
    grid_field = bell_draw(streams_of[0], (CIN, POINTS), 1.0, 6.0, ((1, 128),))
    band_points = set_ends(jax.random.randint(streams_of[1], (N_BAND,), PTS_DEV // 2, PTS_DEV + 1), jax.random.fold_in(streams_of[1], 1), PTS_DEV // 2, PTS_DEV).astype(jnp.int32)
    block_ids = draw_block_ids(jax.random.fold_in(streams_of[12], 71), 0)
    block_count = set_ends(jax.random.randint(streams_of[3], (N_BAND,), K // 2, K + 1), jax.random.fold_in(streams_of[3], 1), K // 2, K).astype(jnp.int32)
    block_weight = jnp.clip(0.039794922 * jax.random.uniform(streams_of[4], (N_BAND, K, NODE_DEV, PBLK), jnp.float32) ** block_levels(streams_of[4], (N_BAND, K, NODE_DEV, PBLK), ((0, 128),), -0.2, 0.2), 0.0, 0.039794922).astype(jnp.bfloat16)
    embed_weight = bell_draw(streams_of[5], (CIN, H), (4 * CIN) ** -0.5, 0.3125, ((1, 2),))
    edge_src = draw_edge_src(jax.random.fold_in(streams_of[12], 71), 0)
    edge_dst = draw_edge_dst(jax.random.fold_in(streams_of[12], 71), 0)
    edge_in_weight = bell_draw(streams_of[8], (2, H, H), H ** -0.5, 0.1875, ((2, 2),))
    edge_out_weight = bell_draw(streams_of[9], (H, H), (8 * H) ** -0.5, 0.0625, ((0, 2),))
    node_in_weight = bell_draw(streams_of[10], (2, H, H), (2 * H) ** -0.5, 0.125, ((2, 2),))
    node_out_weight = bell_draw(streams_of[11], (H, H), H ** -0.5, 0.1875, ((0, 2),))
    return {"grid_field": grid_field, "band_points": band_points, "block_ids": block_ids, "block_count": block_count, "block_weight": block_weight, "embed_weight": embed_weight, "edge_src": edge_src, "edge_dst": edge_dst, "edge_in_weight": edge_in_weight, "edge_out_weight": edge_out_weight, "node_in_weight": node_in_weight, "node_out_weight": node_out_weight}


def reference(grid_field, band_points, block_ids, block_count, block_weight, embed_weight, edge_src, edge_dst, edge_in_weight, edge_out_weight, node_in_weight, node_out_weight):
    column = jnp.arange(POINTS, dtype=jnp.int32)
    limit = band_points[column // PTS_DEV]
    live = jnp.where((column % PTS_DEV < limit)[None, :], grid_field, jnp.zeros_like(grid_field))
    tiles = live.reshape(CIN, POINTS // PBLK, PBLK)

    def remap_band(inputs):
        ids, count, weights = inputs
        blocks = jnp.take(tiles, ids, axis=1)
        live_mask = jnp.arange(K, dtype=jnp.int32) < count
        blocks = jnp.where(live_mask[None, :, None], blocks, jnp.zeros_like(blocks))
        summed = jnp.einsum("knp,ckp->nc", weights.astype(jnp.float32), blocks.astype(jnp.float32))
        return summed.astype(jnp.bfloat16)

    remapped = lax.map(remap_band, (block_ids, block_count, block_weight)).reshape(NODES, CIN)
    initial = jnp.dot(remapped, embed_weight, preferred_element_type=jnp.float32).astype(jnp.bfloat16)
    source_proj = jnp.dot(initial, edge_in_weight[0], preferred_element_type=jnp.float32).astype(jnp.bfloat16)
    target_proj = jnp.dot(initial, edge_in_weight[1], preferred_element_type=jnp.float32).astype(jnp.bfloat16)

    def band_messages(inputs):
        sources, targets = inputs
        pre_act = jnp.take(source_proj, sources, axis=0).astype(jnp.float32) + jnp.take(target_proj, targets, axis=0).astype(jnp.float32)
        edge_hidden = jax.nn.silu(pre_act).astype(jnp.bfloat16)
        messages = jnp.dot(edge_hidden, edge_out_weight, preferred_element_type=jnp.float32)
        return jax.ops.segment_sum(messages, targets % NODE_DEV, num_segments=NODE_DEV)

    aggregate = lax.map(band_messages, (edge_src.reshape(N_BAND, E_DEV), edge_dst.reshape(N_BAND, E_DEV)))
    aggregate = aggregate.reshape(NODES, H).astype(jnp.bfloat16)
    inner = jnp.dot(initial, node_in_weight[0], preferred_element_type=jnp.float32) + jnp.dot(aggregate, node_in_weight[1], preferred_element_type=jnp.float32)
    update = jax.nn.silu(inner).astype(jnp.bfloat16)
    result = initial.astype(jnp.float32) + jnp.dot(update, node_out_weight, preferred_element_type=jnp.float32)
    return result.astype(jnp.bfloat16)
```

```python
import functools

import jax
import jax.numpy as jnp
from jax import lax
from jax.experimental import pallas as pl
from jax.experimental.pallas import tpu as pltpu
from jax.sharding import PartitionSpec as P

F32 = jnp.float32
BF16 = jnp.bfloat16
LANES = 128
VMEM = pl.BlockSpec(memory_space=pltpu.VMEM)
SMEM = pl.BlockSpec(memory_space=pltpu.SMEM)
NT = (((1,), (1,)), ((), ()))
TN = (((0,), (0,)), ((), ()))


def silu(v):
    return v * (0.5 * jnp.tanh(0.5 * v) + 0.5)


def remap_kernel(own, where_ref, ids_ref, count_ref, limit_ref, weight_ref, points_ref, *rest):
    out_ref = rest[-1]
    band, core = where_ref[0], where_ref[1]
    channels = points_ref.shape[0]
    kblocks, _, block_len = weight_ref.shape
    blocks = points_ref.shape[1] // block_len
    if own:
        sub_count = blocks
        out_ref[...] = jnp.zeros_like(out_ref)
    else:
        sub_count = 2 * blocks
        out_ref[...] = rest[0][...]
    for k in range(kblocks):
        local = ids_ref[0, k] - band * sub_count
        live = k < count_ref[0]
        if own:
            mine = (local >= 0) & (local < sub_count) & (core == k % 2)
            block = local
        else:
            low = (core == 0) & (local < 0)
            high = (core == 1) & (local >= sub_count)
            mine = low | high
            block = jnp.where(low, local + blocks, local - sub_count)
        block = jnp.clip(block, 0, blocks - 1)

        @pl.when(live & mine)
        def _():
            at = pl.multiple_of(block * block_len, block_len)
            x = points_ref[:, pl.ds(at, block_len)]
            if own:
                column = at + lax.broadcasted_iota(jnp.int32, x.shape, 1)
                x = jnp.where(column < limit_ref[0], x, jnp.zeros_like(x))
            out_ref[:channels, :] += lax.dot_general(
                x, weight_ref[k], NT, preferred_element_type=F32
            )


def edge_kernel(where_ref, low_ref, mid_ref, high_ref, into_ref, src_ref, dst_ref, out_ref, acc_ref):
    band = where_ref[0]
    nodes = mid_ref.shape[1]
    chunks, size = src_ref.shape
    sources = jnp.concatenate([low_ref[...], mid_ref[...], high_ref[...]], axis=0)
    acc_ref[...] = jnp.zeros_like(acc_ref)

    def step(i, carry):
        src = src_ref[pl.ds(i, 1), :] - (band - 1) * nodes
        dst = dst_ref[pl.ds(i, 1), :] - band * nodes
        piece = src // nodes
        src = src - piece * nodes
        node = lax.broadcasted_iota(jnp.int32, (nodes, size), 0)
        from_hot = (node == src).astype(F32).astype(BF16)
        to_hot = (node == dst).astype(F32).astype(BF16)
        got = jnp.dot(sources, from_hot, preferred_element_type=F32)
        a, b, c = got[:LANES], got[LANES : 2 * LANES], got[2 * LANES :]
        from_src = jnp.where(piece == 0, a, jnp.where(piece == 1, b, c))
        from_dst = jnp.dot(mid_ref[...], to_hot, preferred_element_type=F32)
        both = jnp.concatenate([from_src.astype(BF16), from_dst.astype(BF16)], axis=0)
        pre = jnp.dot(into_ref[...], both, preferred_element_type=F32)
        hidden = silu(pre).astype(BF16)
        acc_ref[...] += lax.dot_general(to_hot, hidden, NT, preferred_element_type=F32)
        return carry

    lax.fori_loop(0, chunks, step, 0)
    out_ref[...] = acc_ref[...].astype(out_ref.dtype)


def update_kernel(where_ref, sums_ref, own_ref, other_ref, mid_ref, direct_ref, out_ref):
    core = where_ref[1]
    v = jnp.dot(sums_ref[core], own_ref[...], preferred_element_type=F32)
    v += jnp.dot(sums_ref[1 - core], other_ref[...], preferred_element_type=F32)
    v += lax.dot_general(mid_ref[...], direct_ref[...], TN, preferred_element_type=F32)
    out_ref[...] = silu(v).astype(out_ref.dtype)


def result_kernel(where_ref, update_ref, own_ref, other_ref, mid_ref, embed_ref, out_ref):
    core = where_ref[1]
    v = jnp.dot(update_ref[core], own_ref[...], preferred_element_type=F32)
    v += jnp.dot(update_ref[1 - core], other_ref[...], preferred_element_type=F32)
    v += lax.dot_general(mid_ref[...], embed_ref[...], TN, preferred_element_type=F32)
    out_ref[...] = v.astype(out_ref.dtype)


def call(kernel, out, specs, limit_mib, flops, args, scratch=()):
    return pl.pallas_call(
        kernel,
        out_shape=out,
        in_specs=specs,
        out_specs=VMEM,
        scratch_shapes=list(scratch),
        compiler_params=pltpu.CompilerParams(vmem_limit_bytes=limit_mib << 20),
        cost_estimate=pl.CostEstimate(flops=flops, bytes_accessed=1 << 20, transcendentals=0),
    )(*args)


def on_device(
    grid_field,
    band_points,
    block_ids,
    block_count,
    block_weight,
    embed_weight,
    edge_src,
    edge_dst,
    edge_in_weight,
    edge_out_weight,
    node_in_weight,
    node_out_weight,
):
    bands = lax.axis_size("band")
    band, core = lax.axis_index("band"), lax.axis_index("ch")
    where = jnp.stack([band, core]).astype(jnp.int32)
    channels, points = grid_field.shape
    _, kblocks, nodes, block_len = block_weight.shape
    share = embed_weight.shape[1]
    half = points // 2
    weight = block_weight[0]

    start = (1 - core) * half
    piece = lax.dynamic_slice_in_dim(grid_field, start, half, 1)
    column = start + lax.broadcasted_iota(jnp.int32, (1, half), 1)
    piece = jnp.where(column < band_points[0], piece, jnp.zeros_like(piece))
    pairs = [(2 * b, 2 * b + 2) for b in range(bands - 1)]
    pairs += [(2 * b + 3, 2 * b + 1) for b in range(bands - 1)]
    halo = lax.ppermute(piece, ("band", "ch"), pairs)

    swap = [(0, 1), (1, 0)]
    embed_full = lax.all_gather(embed_weight, "ch", axis=1, tiled=True)
    out_other = lax.ppermute(edge_out_weight, "ch", swap)
    mine = core * share
    last_own = lax.dynamic_slice_in_dim(node_out_weight, mine, share, 1)
    last_other = lax.ppermute(
        lax.dynamic_slice_in_dim(node_out_weight, share - mine, share, 1), "ch", swap
    )

    def into(w):
        return lax.dot_general(
            w, embed_full, (((0,), (1,)), ((), ())), preferred_element_type=F32
        ).astype(BF16)

    pad = ((0, 0), (0, LANES - channels))
    into_edge = jnp.concatenate(
        [jnp.pad(into(edge_in_weight[0]), pad), jnp.pad(into(edge_in_weight[1]), pad)], axis=1
    )
    direct = jnp.dot(embed_full, node_in_weight[0], preferred_element_type=F32).astype(BF16)
    direct = jnp.pad(direct, (pad[1], pad[0]))
    embed_pad = jnp.pad(embed_weight, (pad[1], pad[0]))
    agg_own = jnp.dot(edge_out_weight, node_in_weight[1], preferred_element_type=F32).astype(BF16)
    agg_other = jnp.dot(out_other, node_in_weight[1], preferred_element_type=F32).astype(BF16)

    sums = jax.ShapeDtypeStruct((LANES, nodes), F32)
    remap_flops = 2 * channels * nodes * block_len * kblocks // 4
    partial = call(
        functools.partial(remap_kernel, True),
        sums,
        [SMEM] * 4 + [VMEM] * 2,
        12,
        remap_flops,
        (where, block_ids, block_count, band_points, weight, grid_field),
    )
    partial = call(
        functools.partial(remap_kernel, False),
        sums,
        [SMEM] * 4 + [VMEM] * 3,
        12,
        remap_flops,
        (where, block_ids, block_count, band_points, weight, halo, partial),
    )
    mid = lax.all_gather(partial, "ch").sum(axis=0).astype(BF16)
    upward = [(b, b + 1) for b in range(bands - 1)]
    low = lax.ppermute(mid, "band", upward)
    high = lax.ppermute(mid, "band", [(t, s) for s, t in upward])

    edges = edge_src.shape[0]
    size = 1024
    by_node = call(
        edge_kernel,
        jax.ShapeDtypeStruct((nodes, share), BF16),
        [SMEM] + [VMEM] * 6,
        20,
        2 * edges * nodes * 7 * 256,
        (
            where,
            low,
            mid,
            high,
            into_edge,
            edge_src.reshape(edges // size, size),
            edge_dst.reshape(edges // size, size),
        ),
        [pltpu.VMEM((nodes, share), F32)],
    )
    by_node = lax.all_gather(by_node, "ch")
    update = call(
        update_kernel,
        jax.ShapeDtypeStruct((nodes, share), BF16),
        [SMEM] + [VMEM] * 5,
        8,
        2 * nodes * share * 2 * share,
        (where, by_node, agg_own, agg_other, mid, direct),
    )
    update = lax.all_gather(update, "ch")
    return call(
        result_kernel,
        jax.ShapeDtypeStruct((nodes, share), BF16),
        [SMEM] + [VMEM] * 5,
        8,
        2 * nodes * share * 2 * share,
        (where, update, last_own, last_other, mid, embed_pad),
    )


def solution(mesh):
    return jax.shard_map(
        on_device,
        mesh=mesh,
        in_specs=(
            P(None, "band"),
            P("band"),
            P("band", None),
            P("band"),
            P("band", None, None, None),
            P(None, "ch"),
            P("band"),
            P("band"),
            P(None, None, "ch"),
            P("ch", None),
            P(None, None, "ch"),
            P("ch", None),
        ),
        out_specs=P("band", "ch"),
        check_vma=False,
    )
```

```python
import jax
import jax.numpy as jnp
from jax import lax
from jax.experimental import pallas as pl
from jax.experimental.pallas import tpu as pltpu
from jax.sharding import PartitionSpec as P

F32 = jnp.float32
BF16 = jnp.bfloat16
VMEM = pl.BlockSpec(memory_space=pltpu.VMEM)
HBM = pl.BlockSpec(memory_space=pltpu.HBM)
SMEM = pl.BlockSpec(memory_space=pltpu.SMEM)
NT = (((1,), (1,)), ((), ()))
TN = (((0,), (0,)), ((), ()))


def silu(v):
    return v * (0.5 * jnp.tanh(0.5 * v) + 0.5)


def pack_kernel(band_points_ref, points_ref, out_ref, limit_ref, limit_sem, sems):
    core = lax.axis_index("ch")
    half = out_ref.shape[1]
    parts = sems.shape[0]
    width = half // parts
    limit_copy = pltpu.make_async_copy(band_points_ref, limit_ref, limit_sem)
    limit_copy.start()
    copies = []
    for i in range(parts):
        start = pl.multiple_of((1 - core) * half + i * width, width)
        copies.append(
            pltpu.make_async_copy(
                points_ref.at[:, pl.ds(start, width)],
                out_ref.at[:, i * width : (i + 1) * width],
                sems.at[i],
            )
        )
        copies[-1].start()
    limit_copy.wait()
    for i in range(parts):
        copies[i].wait()

        @pl.when((core == 0) & (half + (i + 1) * width > limit_ref[0]))
        def _():
            x = out_ref[:, i * width : (i + 1) * width]
            column = half + i * width + lax.broadcasted_iota(jnp.int32, x.shape, 1)
            out_ref[:, i * width : (i + 1) * width] = jnp.where(
                column < limit_ref[0], x, jnp.zeros_like(x)
            )


def own_kernel(
    ids_ref, count_ref, limit_ref, weight_ref, points_ref, out_ref,
):
    band, core = lax.axis_index("band"), lax.axis_index("ch")
    channels = points_ref.shape[0]
    kblocks, _, block_len = weight_ref.shape
    sub_count = points_ref.shape[1] // block_len
    out_ref[...] = jnp.zeros_like(out_ref)
    for k in range(kblocks):
        local = ids_ref[0, k] - band * sub_count
        mine = (local >= 0) & (local < sub_count) & (core == k % 2) & (k < count_ref[0])

        @pl.when(mine)
        def _():
            at = pl.multiple_of(local * block_len, block_len)
            x = points_ref[:, pl.ds(at, block_len)]
            column = at + lax.broadcasted_iota(jnp.int32, x.shape, 1)
            x = jnp.where(column < limit_ref[0], x, jnp.zeros_like(x))
            out_ref[:channels, :] += lax.dot_general(
                x, weight_ref[k], NT, preferred_element_type=F32
            )


def halo_kernel(ids_ref, count_ref, weight_ref, points_ref, own_ref, out_ref, slots):
    band, core = lax.axis_index("band"), lax.axis_index("ch")
    channels = points_ref.shape[0]
    kblocks, _, block_len = weight_ref.shape
    blocks = points_ref.shape[1] // block_len
    sub_count = 2 * blocks
    found = jnp.int32(0)
    for k in range(kblocks):
        local = ids_ref[0, k] - band * sub_count
        low = (core == 0) & (local < 0)
        high = (core == 1) & (local >= sub_count)
        mine = (low | high) & (k < count_ref[0])
        block = jnp.where(low, local + blocks, local - sub_count)

        @pl.when(mine)
        def _():
            slots[0, found] = k
            slots[1, found] = jnp.clip(block, 0, blocks - 1)

        found = found + mine.astype(jnp.int32)
    out_ref[...] = own_ref[...]
    group = 4
    for first in range(0, kblocks, group):

        @pl.when(first < found)
        def _():
            total = None
            for j in range(first, first + group):
                used = j < found
                k = jnp.where(used, slots[0, j], 0)
                block = jnp.where(used, slots[1, j], 0)
                at = pl.multiple_of(block * block_len, block_len)
                x = points_ref[:, pl.ds(at, block_len)]
                x = jnp.where(used, x, jnp.zeros_like(x))
                part = lax.dot_general(x, weight_ref[k], NT, preferred_element_type=F32)
                total = part if total is None else total + part
            out_ref[:channels, :] += total


def weights_kernel(
    embed_ref, embed_other_ref, edge_in_ref, node_own_ref, node_other_ref,
    out_own_ref, out_other_ref, into_ref, direct_ref, agg_ref,
):
    core = lax.axis_index("ch")
    channels, share = embed_ref.shape
    own = pl.ds(pl.multiple_of(core * share, share), share)
    other = pl.ds(pl.multiple_of((1 - core) * share, share), share)

    def dot(a, b):
        return jnp.dot(a, b, preferred_element_type=F32)

    rows = direct_ref.shape[0]
    into_ref[...] = jnp.zeros_like(into_ref)
    direct_ref[...] = jnp.zeros_like(direct_ref)
    for i in range(2):
        v = dot(embed_ref[...], edge_in_ref[i, own, :])
        v += dot(embed_other_ref[...], edge_in_ref[i, other, :])
        into_ref[i * rows : i * rows + channels, :] = v.astype(BF16)
    for j, node_ref in enumerate((node_own_ref, node_other_ref)):
        columns = slice(j * share, (j + 1) * share)
        v = dot(embed_ref[...], node_ref[0, own, :])
        v += dot(embed_other_ref[...], node_ref[0, other, :])
        direct_ref[:channels, columns] = v.astype(BF16)
        for i, half_ref in enumerate((out_own_ref, out_other_ref)):
            agg_ref[i, :, columns] = dot(half_ref[...], node_ref[1]).astype(BF16)


def edge_kernel(near_ref, mid_ref, into_ref, src_ref, dst_ref, out_ref, acc_ref):
    band = lax.axis_index("band")
    rows, nodes = mid_ref.shape
    edges = src_ref.shape[1]
    size = edges // 2
    sources = jnp.concatenate([near_ref[0], mid_ref[...], near_ref[1]], axis=0)
    node = lax.broadcasted_iota(jnp.int32, (nodes, size), 0).astype(F32).astype(BF16)
    one, zero = jnp.ones((), BF16), jnp.zeros((), BF16)

    def before(at):
        src = src_ref[:, at : at + size] - (band - 1) * nodes
        dst = dst_ref[:, at : at + size] - band * nodes
        piece = src // nodes
        from_hot = jnp.where(node == (src - piece * nodes).astype(F32).astype(BF16), one, zero)
        to_hot = jnp.where(node == dst.astype(F32).astype(BF16), one, zero)
        got = jnp.dot(sources, from_hot, preferred_element_type=F32)
        a, b, c = got[:rows], got[rows : 2 * rows], got[2 * rows :]
        from_src = jnp.where(piece == 0, a, jnp.where(piece == 1, b, c))
        from_dst = jnp.dot(mid_ref[...], to_hot, preferred_element_type=F32)
        both = jnp.concatenate([from_src.astype(BF16), from_dst.astype(BF16)], axis=0)
        return lax.dot_general(into_ref[...], both, TN, preferred_element_type=F32), to_hot

    acc_ref[...] = jnp.zeros_like(acc_ref)
    now = before(0)
    for at in range(0, edges, size):
        later = before(at + size) if at + size < edges else None
        pre, to_hot = now
        hidden = silu(pre).astype(BF16)
        acc_ref[...] += lax.dot_general(to_hot, hidden, NT, preferred_element_type=F32)
        now = later
    out_ref[...] = acc_ref[...].astype(out_ref.dtype)


def node_kernel(
    sums_ref, mid_ref, direct_ref, embed_ref, agg_hbm, last_own_hbm, last_other_hbm, out_ref,
    agg_ref, last_ref, sems,
):
    core = lax.axis_index("ch")
    channels, share = embed_ref.shape
    columns = pl.ds(pl.multiple_of(core * share, share), share)
    copies = [
        pltpu.make_async_copy(agg_hbm.at[0], agg_ref.at[0], sems.at[0]),
        pltpu.make_async_copy(agg_hbm.at[1], agg_ref.at[1], sems.at[1]),
        pltpu.make_async_copy(last_own_hbm.at[:, columns], last_ref.at[0], sems.at[2]),
        pltpu.make_async_copy(last_other_hbm.at[:, columns], last_ref.at[1], sems.at[3]),
    ]
    for copy in copies:
        copy.start()
    v = lax.dot_general(mid_ref[...], direct_ref[...], TN, preferred_element_type=F32)
    copies[0].wait()
    v += jnp.dot(sums_ref[core], agg_ref[0], preferred_element_type=F32)
    copies[1].wait()
    v += jnp.dot(sums_ref[1 - core], agg_ref[1], preferred_element_type=F32)
    update = silu(v).astype(BF16)
    v = lax.dot_general(mid_ref[:channels, :], embed_ref[...], TN, preferred_element_type=F32)
    copies[2].wait()
    v += jnp.dot(update[:, :share], last_ref[0], preferred_element_type=F32)
    copies[3].wait()
    v += jnp.dot(update[:, share:], last_ref[1], preferred_element_type=F32)
    out_ref[...] = v.astype(out_ref.dtype)


def call(kernel, out, specs, limit_mib, flops, args, scratch=()):
    return pl.pallas_call(
        kernel,
        out_shape=out,
        in_specs=specs,
        out_specs=[VMEM] * len(out) if isinstance(out, tuple) else VMEM,
        scratch_shapes=list(scratch),
        compiler_params=pltpu.CompilerParams(vmem_limit_bytes=int(limit_mib * 2**20)),
        cost_estimate=pl.CostEstimate(flops=flops, bytes_accessed=1 << 20, transcendentals=0),
    )(*args)


def on_device(
    grid_field,
    band_points,
    block_ids,
    block_count,
    block_weight,
    embed_weight,
    edge_src,
    edge_dst,
    edge_in_weight,
    edge_out_weight,
    node_in_weight,
    node_out_weight,
):
    bands = lax.axis_size("band")
    channels, points = grid_field.shape
    _, kblocks, nodes, block_len = block_weight.shape
    share = embed_weight.shape[1]
    edges = edge_src.shape[0]
    half = points // 2
    rows = -(-channels // 16) * 16
    weight = block_weight[0]
    shape = jax.ShapeDtypeStruct

    pairs = [(2 * b, 2 * b + 2) for b in range(bands - 1)]
    pairs += [(2 * b + 3, 2 * b + 1) for b in range(bands - 1)]
    piece = call(
        pack_kernel,
        pltpu.VMEM((channels, half), BF16),
        [HBM, HBM],
        61,
        1 << 20,
        (band_points, grid_field),
        [pltpu.SMEM((1,), jnp.int32), pltpu.SemaphoreType.DMA, pltpu.SemaphoreType.DMA((8,))],
    )
    halo = lax.ppermute(piece, ("band", "ch"), pairs)

    def partner(x):
        return lax.ppermute(x, "ch", [(0, 1), (1, 0)])

    embed_other = partner(embed_weight)
    out_other = partner(edge_out_weight)
    node_other = partner(node_in_weight)
    last_other = partner(node_out_weight)
    src, dst = edge_src.reshape(1, edges), edge_dst.reshape(1, edges)
    remap_flops = 2 * channels * nodes * block_len * kblocks // 4
    sums = shape((rows, nodes), F32)
    partial = call(
        own_kernel,
        sums,
        [SMEM] * 3 + [VMEM] * 2,
        16,
        8 * remap_flops,
        (block_ids, block_count, band_points, weight, grid_field),
    )
    into_edge, direct, agg = call(
        weights_kernel,
        (
            shape((2 * rows, share), BF16),
            shape((rows, 2 * share), BF16),
            shape((2, share, 2 * share), BF16),
        ),
        [VMEM] * 7,
        16,
        16 * share**3,
        (
            embed_weight,
            embed_other,
            edge_in_weight,
            node_in_weight,
            node_other,
            edge_out_weight,
            out_other,
        ),
    )

    partial = call(
        halo_kernel,
        sums,
        [SMEM] * 2 + [VMEM] * 3,
        12,
        remap_flops,
        (block_ids, block_count, weight, halo, partial),
        [pltpu.SMEM((2, kblocks), jnp.int32)],
    )
    mid = lax.all_gather(partial, "ch").sum(axis=0).astype(BF16)
    near = lax.ppermute(mid, ("band", "ch"), pairs)
    near = lax.all_gather(near, "ch")
    by_node = call(
        edge_kernel,
        shape((nodes, share), BF16),
        [VMEM] * 5,
        24,
        2 * edges * nodes * 7 * 256,
        (near, mid, into_edge, src, dst),
        [pltpu.VMEM((nodes, share), F32)],
    )
    return call(
        node_kernel,
        shape((nodes, share), BF16),
        [VMEM] * 4 + [HBM] * 3,
        61,
        2 * nodes * share * 6 * share,
        (
            lax.all_gather(by_node, "ch"),
            mid,
            direct,
            embed_weight,
            agg,
            node_out_weight,
            last_other,
        ),
        [
            pltpu.VMEM((2, share, 2 * share), BF16),
            pltpu.VMEM((2, share, share), BF16),
            pltpu.SemaphoreType.DMA((4,)),
        ],
    )


def solution(mesh):
    return jax.shard_map(
        on_device,
        mesh=mesh,
        in_specs=(
            P(None, "band"),
            P("band"),
            P("band", None),
            P("band"),
            P("band", None, None, None),
            P(None, "ch"),
            P("band"),
            P("band"),
            P(None, None, "ch"),
            P("ch", None),
            P(None, None, "ch"),
            P("ch", None),
        ),
        out_specs=P("band", "ch"),
        check_vma=False,
    )
```

```python
import jax
import jax.numpy as jnp
from jax import lax
from jax.experimental import pallas as pl
from jax.experimental.pallas import tpu as pltpu
from jax.sharding import PartitionSpec as P

F32 = jnp.float32
BF16 = jnp.bfloat16
VMEM = pl.BlockSpec(memory_space=pltpu.VMEM)
HBM = pl.BlockSpec(memory_space=pltpu.HBM)
SMEM = pl.BlockSpec(memory_space=pltpu.SMEM)
NT = (((1,), (1,)), ((), ()))
TN = (((0,), (0,)), ((), ()))


def silu(v):
    return v * (0.5 * jnp.tanh(0.5 * v) + 0.5)


def pack_kernel(band_points_ref, points_ref, out_ref, limit_ref, limit_sem, sems):
    core = lax.axis_index("ch")
    half = out_ref.shape[1]
    parts = sems.shape[0]
    width = half // parts
    limit_copy = pltpu.make_async_copy(band_points_ref, limit_ref, limit_sem)
    limit_copy.start()
    copies = []
    for i in range(parts):
        start = pl.multiple_of((1 - core) * half + i * width, width)
        copies.append(
            pltpu.make_async_copy(
                points_ref.at[:, pl.ds(start, width)],
                out_ref.at[:, i * width : (i + 1) * width],
                sems.at[i],
            )
        )
        copies[-1].start()
    limit_copy.wait()
    for i in range(parts):
        copies[i].wait()

        @pl.when((core == 0) & (half + (i + 1) * width > limit_ref[0]))
        def _():
            x = out_ref[:, i * width : (i + 1) * width]
            column = half + i * width + lax.broadcasted_iota(jnp.int32, x.shape, 1)
            out_ref[:, i * width : (i + 1) * width] = jnp.where(
                column < limit_ref[0], x, jnp.zeros_like(x)
            )


def own_kernel(
    ids_ref, count_ref, limit_ref, weight_ref, points_ref, out_ref,
):
    band, core = lax.axis_index("band"), lax.axis_index("ch")
    channels = points_ref.shape[0]
    kblocks, _, block_len = weight_ref.shape
    sub_count = points_ref.shape[1] // block_len
    out_ref[...] = jnp.zeros_like(out_ref)
    for k in range(kblocks):
        local = ids_ref[0, k] - band * sub_count
        mine = (local >= 0) & (local < sub_count) & (core == k % 2) & (k < count_ref[0])

        @pl.when(mine)
        def _():
            at = pl.multiple_of(local * block_len, block_len)
            x = points_ref[:, pl.ds(at, block_len)]
            column = at + lax.broadcasted_iota(jnp.int32, x.shape, 1)
            x = jnp.where(column < limit_ref[0], x, jnp.zeros_like(x))
            out_ref[:channels, :] += lax.dot_general(
                x, weight_ref[k], NT, preferred_element_type=F32
            )


def halo_kernel(ids_ref, count_ref, weight_ref, points_ref, own_ref, out_ref, slots):
    band, core = lax.axis_index("band"), lax.axis_index("ch")
    channels = points_ref.shape[0]
    kblocks, _, block_len = weight_ref.shape
    blocks = points_ref.shape[1] // block_len
    sub_count = 2 * blocks
    found = jnp.int32(0)
    for k in range(kblocks):
        local = ids_ref[0, k] - band * sub_count
        low = (core == 0) & (local < 0)
        high = (core == 1) & (local >= sub_count)
        mine = (low | high) & (k < count_ref[0])
        block = jnp.where(low, local + blocks, local - sub_count)

        @pl.when(mine)
        def _():
            slots[0, found] = k
            slots[1, found] = jnp.clip(block, 0, blocks - 1)

        found = found + mine.astype(jnp.int32)
    out_ref[...] = own_ref[...]
    group = 4
    for first in range(0, kblocks, group):

        @pl.when(first < found)
        def _():
            total = None
            for j in range(first, first + group):
                used = j < found
                k = jnp.where(used, slots[0, j], 0)
                block = jnp.where(used, slots[1, j], 0)
                at = pl.multiple_of(block * block_len, block_len)
                x = points_ref[:, pl.ds(at, block_len)]
                x = jnp.where(used, x, jnp.zeros_like(x))
                part = lax.dot_general(x, weight_ref[k], NT, preferred_element_type=F32)
                total = part if total is None else total + part
            out_ref[:channels, :] += total


def weights_kernel(
    embed_ref, embed_other_ref, edge_in_ref, node_own_ref, node_other_ref,
    out_own_ref, out_other_ref, last_own_hbm, last_other_hbm,
    into_ref, direct_ref, agg_ref, last_ref, sems,
):
    core = lax.axis_index("ch")
    channels, share = embed_ref.shape
    own = pl.ds(pl.multiple_of(core * share, share), share)
    other = pl.ds(pl.multiple_of((1 - core) * share, share), share)

    copies = [
        pltpu.make_async_copy(half.at[:, own], last_ref.at[i], sems.at[i])
        for i, half in enumerate((last_own_hbm, last_other_hbm))
    ]
    for copy in copies:
        copy.start()

    def dot(a, b):
        return jnp.dot(a, b, preferred_element_type=F32)

    rows = direct_ref.shape[0]
    into_ref[...] = jnp.zeros_like(into_ref)
    direct_ref[...] = jnp.zeros_like(direct_ref)
    for i in range(2):
        v = dot(embed_ref[...], edge_in_ref[i, own, :])
        v += dot(embed_other_ref[...], edge_in_ref[i, other, :])
        into_ref[i * rows : i * rows + channels, :] = v.astype(BF16)
    for j, node_ref in enumerate((node_own_ref, node_other_ref)):
        columns = slice(j * share, (j + 1) * share)
        v = dot(embed_ref[...], node_ref[0, own, :])
        v += dot(embed_other_ref[...], node_ref[0, other, :])
        direct_ref[:channels, columns] = v.astype(BF16)
        for i, half_ref in enumerate((out_own_ref, out_other_ref)):
            agg_ref[i, :, columns] = dot(half_ref[...], node_ref[1]).astype(BF16)
    for copy in copies:
        copy.wait()


def edge_kernel(near_ref, other_ref, mid_ref, into_ref, src_ref, dst_ref, out_ref, acc_ref):
    band = lax.axis_index("band")
    rows, nodes = mid_ref.shape
    edges = src_ref.shape[1]
    size = edges // 2
    first = lax.axis_index("ch") == 0
    low = jnp.where(first, near_ref[...], other_ref[...])
    high = jnp.where(first, other_ref[...], near_ref[...])
    sources = jnp.concatenate([low, mid_ref[...], high], axis=0)
    node = lax.broadcasted_iota(jnp.int32, (nodes, size), 0).astype(F32).astype(BF16)
    one, zero = jnp.ones((), BF16), jnp.zeros((), BF16)

    def before(at):
        src = src_ref[:, at : at + size] - (band - 1) * nodes
        dst = dst_ref[:, at : at + size] - band * nodes
        piece = src // nodes
        from_hot = jnp.where(node == (src - piece * nodes).astype(F32).astype(BF16), one, zero)
        to_hot = jnp.where(node == dst.astype(F32).astype(BF16), one, zero)
        got = jnp.dot(sources, from_hot, preferred_element_type=F32)
        a, b, c = got[:rows], got[rows : 2 * rows], got[2 * rows :]
        from_src = jnp.where(piece == 0, a, jnp.where(piece == 1, b, c))
        from_dst = jnp.dot(mid_ref[...], to_hot, preferred_element_type=F32)
        both = jnp.concatenate([from_src.astype(BF16), from_dst.astype(BF16)], axis=0)
        return lax.dot_general(into_ref[...], both, TN, preferred_element_type=F32), to_hot

    acc_ref[...] = jnp.zeros_like(acc_ref)
    now = before(0)
    for at in range(0, edges, size):
        later = before(at + size) if at + size < edges else None
        pre, to_hot = now
        hidden = silu(pre).astype(BF16)
        acc_ref[...] += lax.dot_general(to_hot, hidden, NT, preferred_element_type=F32)
        now = later
    out_ref[...] = acc_ref[...].astype(out_ref.dtype)


def node_kernel(own_ref, other_ref, mid_ref, direct_ref, embed_ref, agg_ref, last_ref, out_ref):
    channels, share = embed_ref.shape
    v = lax.dot_general(mid_ref[...], direct_ref[...], TN, preferred_element_type=F32)
    v += jnp.dot(own_ref[...], agg_ref[0], preferred_element_type=F32)
    v += jnp.dot(other_ref[...], agg_ref[1], preferred_element_type=F32)
    update = silu(v).astype(BF16)
    v = lax.dot_general(mid_ref[:channels, :], embed_ref[...], TN, preferred_element_type=F32)
    v += jnp.dot(update[:, :share], last_ref[0], preferred_element_type=F32)
    v += jnp.dot(update[:, share:], last_ref[1], preferred_element_type=F32)
    out_ref[...] = v.astype(out_ref.dtype)


def call(kernel, out, specs, limit_mib, flops, args, scratch=()):
    return pl.pallas_call(
        kernel,
        out_shape=out,
        in_specs=specs,
        out_specs=[VMEM] * len(out) if isinstance(out, tuple) else VMEM,
        scratch_shapes=list(scratch),
        compiler_params=pltpu.CompilerParams(vmem_limit_bytes=int(limit_mib * 2**20)),
        cost_estimate=pl.CostEstimate(flops=flops, bytes_accessed=1 << 20, transcendentals=0),
    )(*args)


def on_device(
    grid_field,
    band_points,
    block_ids,
    block_count,
    block_weight,
    embed_weight,
    edge_src,
    edge_dst,
    edge_in_weight,
    edge_out_weight,
    node_in_weight,
    node_out_weight,
):
    bands = lax.axis_size("band")
    channels, points = grid_field.shape
    _, kblocks, nodes, block_len = block_weight.shape
    share = embed_weight.shape[1]
    edges = edge_src.shape[0]
    half = points // 2
    rows = -(-channels // 16) * 16
    weight = block_weight[0]
    shape = jax.ShapeDtypeStruct

    pairs = [(2 * b, 2 * b + 2) for b in range(bands - 1)] + [(2 * bands - 2, 2 * bands - 1)]
    pairs += [(2 * b + 3, 2 * b + 1) for b in range(bands - 1)] + [(1, 0)]
    piece = call(
        pack_kernel,
        pltpu.VMEM((channels, half), BF16),
        [HBM, HBM],
        61,
        1 << 20,
        (band_points, grid_field),
        [pltpu.SMEM((1,), jnp.int32), pltpu.SemaphoreType.DMA, pltpu.SemaphoreType.DMA((8,))],
    )
    halo = lax.ppermute(piece, ("band", "ch"), pairs)

    def partner(x):
        return lax.ppermute(x, "ch", [(0, 1), (1, 0)])

    embed_other = partner(embed_weight)
    out_other = partner(edge_out_weight)
    node_other = partner(node_in_weight)
    last_other = partner(node_out_weight)
    src, dst = edge_src.reshape(1, edges), edge_dst.reshape(1, edges)
    remap_flops = 2 * channels * nodes * block_len * kblocks // 4
    sums = shape((rows, nodes), F32)
    partial = call(
        own_kernel,
        sums,
        [SMEM] * 3 + [VMEM] * 2,
        16,
        8 * remap_flops,
        (block_ids, block_count, band_points, weight, grid_field),
    )
    into_edge, direct, agg, last = call(
        weights_kernel,
        (
            shape((2 * rows, share), BF16),
            shape((rows, 2 * share), BF16),
            shape((2, share, 2 * share), BF16),
            shape((2, share, share), BF16),
        ),
        [VMEM] * 7 + [HBM] * 2,
        18,
        16 * share**3,
        (
            embed_weight,
            embed_other,
            edge_in_weight,
            node_in_weight,
            node_other,
            edge_out_weight,
            out_other,
            node_out_weight,
            last_other,
        ),
        [pltpu.SemaphoreType.DMA((2,))],
    )

    partial = call(
        halo_kernel,
        sums,
        [SMEM] * 2 + [VMEM] * 3,
        12,
        remap_flops,
        (block_ids, block_count, weight, halo, partial),
        [pltpu.SMEM((2, kblocks), jnp.int32)],
    )
    mid = (partial + partner(partial)).astype(BF16)
    near = lax.ppermute(mid, ("band", "ch"), pairs)
    near_other = partner(near)
    by_node = call(
        edge_kernel,
        shape((nodes, share), BF16),
        [VMEM] * 6,
        24,
        2 * edges * nodes * 7 * 256,
        (near, near_other, mid, into_edge, src, dst),
        [pltpu.VMEM((nodes, share), F32)],
    )
    return call(
        node_kernel,
        shape((nodes, share), BF16),
        [VMEM] * 7,
        12,
        2 * nodes * share * 6 * share,
        (by_node, partner(by_node), mid, direct, embed_weight, agg, last),
    )


def solution(mesh):
    return jax.shard_map(
        on_device,
        mesh=mesh,
        in_specs=(
            P(None, "band"),
            P("band"),
            P("band", None),
            P("band"),
            P("band", None, None, None),
            P(None, "ch"),
            P("band"),
            P("band"),
            P(None, None, "ch"),
            P("ch", None),
            P(None, None, "ch"),
            P("ch", None),
        ),
        out_specs=P("band", "ch"),
        check_vma=False,
    )
```

```python
import functools

import jax
import jax.numpy as jnp
from jax import lax
from jax.experimental import pallas as pl
from jax.experimental.pallas import tpu as pltpu
from jax.sharding import PartitionSpec as P

F32 = jnp.float32
BF16 = jnp.bfloat16
VMEM = pl.BlockSpec(memory_space=pltpu.VMEM)
HBM = pl.BlockSpec(memory_space=pltpu.HBM)
SMEM = pl.BlockSpec(memory_space=pltpu.SMEM)
NT = (((1,), (1,)), ((), ()))
TN = (((0,), (0,)), ((), ()))


def silu(v):
    return v * (0.5 * jnp.tanh(0.5 * v) + 0.5)


def pack_kernel(band_points_ref, points_ref, out_ref, rows_ref, limit_ref, limit_sem, sems):
    core = lax.axis_index("ch")
    channels, half = rows_ref.shape
    parts = sems.shape[0]
    width = half // parts
    limit_copy = pltpu.make_async_copy(band_points_ref, limit_ref, limit_sem)
    limit_copy.start()
    copies = []
    for i in range(parts):
        start = pl.multiple_of((1 - core) * half + i * width, width)
        copies.append(
            pltpu.make_async_copy(
                points_ref.at[:, pl.ds(start, width)],
                rows_ref.at[:, i * width : (i + 1) * width],
                sems.at[i],
            )
        )
        copies[-1].start()
    limit_copy.wait()
    limit = jnp.where(core == 0, limit_ref[0] - half, half)
    full = channels // 8
    last = channels - 8 * full
    for i in range(parts):
        copies[i].wait()
        at = i * width
        live = at + lax.broadcasted_iota(jnp.int32, (8, width), 1) < limit
        for t in range(full):
            x = rows_ref[8 * t : 8 * t + 8, at : at + width]
            out_ref[:, t * half + at : t * half + at + width] = jnp.where(live, x, jnp.zeros_like(x))
        x = rows_ref[8 * full :, at : at + width]
        x = jnp.where(live[:last], x, jnp.zeros_like(x))
        low = at % (half * last // 8)
        row = (at // (half * last // 8)) * last
        out_ref[row : row + last, full * half + low : full * half + low + width] = x


def own_kernel(
    ids_ref, count_ref, limit_ref, weight_ref, points_ref, out_ref,
):
    band, core = lax.axis_index("band"), lax.axis_index("ch")
    channels = points_ref.shape[0]
    kblocks, _, block_len = weight_ref.shape
    sub_count = points_ref.shape[1] // block_len
    out_ref[...] = jnp.zeros_like(out_ref)
    for k in range(kblocks):
        local = ids_ref[0, k] - band * sub_count
        mine = (local >= 0) & (local < sub_count) & (core == k % 2) & (k < count_ref[0])

        @pl.when(mine)
        def _():
            at = pl.multiple_of(local * block_len, block_len)
            x = points_ref[:, pl.ds(at, block_len)]
            column = at + lax.broadcasted_iota(jnp.int32, x.shape, 1)
            x = jnp.where(column < limit_ref[0], x, jnp.zeros_like(x))
            out_ref[:channels, :] += lax.dot_general(
                x, weight_ref[k], NT, preferred_element_type=F32
            )


def hots_kernel(src_ref, dst_ref, from_ref, to_ref):
    band = lax.axis_index("band")
    nodes, edges = from_ref.shape
    size = edges // 10
    node = lax.broadcasted_iota(jnp.int32, (nodes, size), 0).astype(F32).astype(BF16)
    one, zero = jnp.ones((), BF16), jnp.zeros((), BF16)
    for at in range(0, edges, size):
        src = src_ref[:, at : at + size] - (band - 1) * nodes
        src = src - (src // nodes) * nodes
        dst = dst_ref[:, at : at + size] - band * nodes
        from_ref[:, at : at + size] = jnp.where(node == src.astype(F32).astype(BF16), one, zero)
        to_ref[:, at : at + size] = jnp.where(node == dst.astype(F32).astype(BF16), one, zero)


def gather_kernel(mid_ref, src_ref, from_ref, to_ref, out_ref):
    band = lax.axis_index("band")
    rows, nodes = mid_ref.shape
    edges = src_ref.shape[1]
    size = edges // 2
    for at in range(0, edges, size):
        piece = (src_ref[:, at : at + size] - (band - 1) * nodes) // nodes
        got = jnp.dot(mid_ref[...], from_ref[:, at : at + size], preferred_element_type=F32)
        out_ref[:rows, at : at + size] = jnp.where(piece == 1, got, 0.0).astype(BF16)
        got = jnp.dot(mid_ref[...], to_ref[:, at : at + size], preferred_element_type=F32)
        out_ref[rows:, at : at + size] = got.astype(BF16)


def halo_kernel(channels, ids_ref, count_ref, weight_ref, points_ref, own_ref, out_ref, slots):
    band, core = lax.axis_index("band"), lax.axis_index("ch")
    kblocks, _, block_len = weight_ref.shape
    half = points_ref.shape[1] * 8 // channels
    blocks = half // block_len
    sub_count = 2 * blocks
    full = channels // 8
    last = channels - 8 * full
    found = jnp.int32(0)
    for k in range(kblocks):
        local = ids_ref[0, k] - band * sub_count
        low = (core == 0) & (local < 0)
        high = (core == 1) & (local >= sub_count)
        mine = (low | high) & (k < count_ref[0])
        block = jnp.where(low, local + blocks, local - sub_count)

        @pl.when(mine)
        def _():
            slots[0, found] = k
            slots[1, found] = jnp.clip(block, 0, blocks - 1)

        found = found + mine.astype(jnp.int32)
    out_ref[...] = own_ref[...]
    group = 4
    for first in range(0, kblocks, group):

        @pl.when(first < found)
        def _():
            total = None
            for j in range(first, first + group):
                used = j < found
                k = jnp.where(used, slots[0, j], 0)
                block = jnp.where(used, slots[1, j], 0)
                at = pl.multiple_of(block * block_len, block_len)
                x = [
                    points_ref[:, pl.ds(pl.multiple_of(t * half + at, block_len), block_len)]
                    for t in range(full)
                ]
                stack = half * last // 8
                low = pl.multiple_of(full * half + lax.rem(at, stack), block_len)
                tail = points_ref[:, pl.ds(low, block_len)].astype(F32)
                tail = jnp.where(at < stack, tail[:last], tail[last : 2 * last])
                x = jnp.concatenate([piece.astype(F32) for piece in x] + [tail], axis=0)
                x = jnp.where(used, x, 0.0).astype(BF16)
                part = lax.dot_general(x, weight_ref[k], NT, preferred_element_type=F32)
                total = part if total is None else total + part
            out_ref[:channels, :] += total


def weights_kernel(
    embed_ref, embed_other_ref, edge_in_ref, node_own_ref, node_other_ref,
    out_own_ref, out_other_ref, last_own_hbm, last_other_hbm,
    into_ref, direct_ref, agg_ref, last_ref, sems,
):
    core = lax.axis_index("ch")
    channels, share = embed_ref.shape
    own = pl.ds(pl.multiple_of(core * share, share), share)
    other = pl.ds(pl.multiple_of((1 - core) * share, share), share)

    copies = [
        pltpu.make_async_copy(half.at[:, own], last_ref.at[i], sems.at[i])
        for i, half in enumerate((last_own_hbm, last_other_hbm))
    ]
    for copy in copies:
        copy.start()

    def dot(a, b):
        return jnp.dot(a, b, preferred_element_type=F32)

    rows = direct_ref.shape[0]
    into_ref[...] = jnp.zeros_like(into_ref)
    direct_ref[...] = jnp.zeros_like(direct_ref)
    for i in range(2):
        v = dot(embed_ref[...], edge_in_ref[i, own, :])
        v += dot(embed_other_ref[...], edge_in_ref[i, other, :])
        into_ref[i * rows : i * rows + channels, :] = v.astype(BF16)
    for j, node_ref in enumerate((node_own_ref, node_other_ref)):
        columns = slice(j * share, (j + 1) * share)
        v = dot(embed_ref[...], node_ref[0, own, :])
        v += dot(embed_other_ref[...], node_ref[0, other, :])
        direct_ref[:channels, columns] = v.astype(BF16)
        for i, half_ref in enumerate((out_own_ref, out_other_ref)):
            agg_ref[i, :, columns] = dot(half_ref[...], node_ref[1]).astype(BF16)
    for copy in copies:
        copy.wait()


def edge_kernel(
    near_ref, far_ref, into_ref, src_ref, from_ref, to_ref, gathered_ref, out_ref, acc_ref
):
    band = lax.axis_index("band")
    rows, nodes = near_ref.shape
    edges = src_ref.shape[1]
    size = edges // 2
    even = lax.rem(band, 2) == 0
    low = jnp.where(even, far_ref[...], near_ref[...])
    high = jnp.where(even, near_ref[...], far_ref[...])
    sources = jnp.concatenate([low, high], axis=0)

    def before(at):
        piece = (src_ref[:, at : at + size] - (band - 1) * nodes) // nodes
        got = jnp.dot(sources, from_ref[:, at : at + size], preferred_element_type=F32)
        got = jnp.where(piece == 0, got[:rows], jnp.where(piece == 2, got[rows:], 0.0))
        from_src = got.astype(BF16) + gathered_ref[:rows, at : at + size]
        both = jnp.concatenate([from_src, gathered_ref[rows:, at : at + size]], axis=0)
        return lax.dot_general(into_ref[...], both, TN, preferred_element_type=F32)

    acc_ref[...] = jnp.zeros_like(acc_ref)
    now = before(0)
    for at in range(0, edges, size):
        later = before(at + size) if at + size < edges else None
        hidden = silu(now.astype(BF16))
        acc_ref[...] += lax.dot_general(
            to_ref[:, at : at + size], hidden, NT, preferred_element_type=F32
        )
        now = later
    out_ref[...] = acc_ref[...].astype(out_ref.dtype)


def node_kernel(own_ref, other_ref, mid_ref, direct_ref, embed_ref, agg_ref, last_ref, out_ref):
    channels, share = embed_ref.shape
    v = lax.dot_general(mid_ref[...], direct_ref[...], TN, preferred_element_type=F32)
    v += jnp.dot(own_ref[...], agg_ref[0], preferred_element_type=F32)
    v += jnp.dot(other_ref[...], agg_ref[1], preferred_element_type=F32)
    update = silu(v).astype(BF16)
    v = lax.dot_general(mid_ref[:channels, :], embed_ref[...], TN, preferred_element_type=F32)
    v += jnp.dot(update[:, :share], last_ref[0], preferred_element_type=F32)
    v += jnp.dot(update[:, share:], last_ref[1], preferred_element_type=F32)
    out_ref[...] = v.astype(out_ref.dtype)


def call(kernel, out, specs, limit_mib, flops, args, scratch=()):
    return pl.pallas_call(
        kernel,
        out_shape=out,
        in_specs=specs,
        out_specs=[VMEM] * len(out) if isinstance(out, tuple) else VMEM,
        scratch_shapes=list(scratch),
        compiler_params=pltpu.CompilerParams(vmem_limit_bytes=int(limit_mib * 2**20)),
        cost_estimate=pl.CostEstimate(flops=flops, bytes_accessed=1 << 20, transcendentals=0),
    )(*args)


def on_device(
    grid_field,
    band_points,
    block_ids,
    block_count,
    block_weight,
    embed_weight,
    edge_src,
    edge_dst,
    edge_in_weight,
    edge_out_weight,
    node_in_weight,
    node_out_weight,
):
    bands = lax.axis_size("band")
    channels, points = grid_field.shape
    _, kblocks, nodes, block_len = block_weight.shape
    share = embed_weight.shape[1]
    edges = edge_src.shape[0]
    half = points // 2
    rows = -(-channels // 16) * 16
    weight = block_weight[0]
    shape = jax.ShapeDtypeStruct

    pairs = [(2 * b, 2 * b + 2) for b in range(bands - 1)] + [(2 * bands - 2, 2 * bands - 1)]
    pairs += [(2 * b + 3, 2 * b + 1) for b in range(bands - 1)] + [(1, 0)]
    piece = call(
        pack_kernel,
        pltpu.VMEM((8, channels * half // 8), BF16),
        [HBM, HBM],
        61,
        1 << 20,
        (band_points, grid_field),
        [
            pltpu.VMEM((channels, half), BF16),
            pltpu.SMEM((1,), jnp.int32),
            pltpu.SemaphoreType.DMA,
            pltpu.SemaphoreType.DMA((8,)),
        ],
    )
    halo = lax.ppermute(piece, ("band", "ch"), pairs)

    def partner(x):
        return lax.ppermute(x, "ch", [(0, 1), (1, 0)])

    embed_other = partner(embed_weight)
    out_other = partner(edge_out_weight)
    node_other = partner(node_in_weight)
    last_other = partner(node_out_weight)
    src, dst = edge_src.reshape(1, edges), edge_dst.reshape(1, edges)
    remap_flops = 2 * channels * nodes * block_len * kblocks // 4
    sums = shape((rows, nodes), F32)
    partial = call(
        own_kernel,
        sums,
        [SMEM] * 3 + [VMEM] * 2,
        16,
        8 * remap_flops,
        (block_ids, block_count, band_points, weight, grid_field),
    )
    from_hot, to_hot = call(
        hots_kernel,
        (shape((nodes, edges), BF16), shape((nodes, edges), BF16)),
        [VMEM] * 2,
        4,
        edges * nodes * 16,
        (src, dst),
    )
    into_edge, direct, agg, last = call(
        weights_kernel,
        (
            shape((2 * rows, share), BF16),
            shape((rows, 2 * share), BF16),
            shape((2, share, 2 * share), BF16),
            shape((2, share, share), BF16),
        ),
        [VMEM] * 7 + [HBM] * 2,
        18,
        16 * share**3,
        (
            embed_weight,
            embed_other,
            edge_in_weight,
            node_in_weight,
            node_other,
            edge_out_weight,
            out_other,
            node_out_weight,
            last_other,
        ),
        [pltpu.SemaphoreType.DMA((2,))],
    )

    partial = call(
        functools.partial(halo_kernel, channels),
        sums,
        [SMEM] * 2 + [VMEM] * 3,
        12,
        remap_flops,
        (block_ids, block_count, weight, halo, partial),
        [pltpu.SMEM((2, kblocks), jnp.int32)],
    )
    mid = (partial + partner(partial)).astype(BF16)

    def exchange(first):
        ups = [(b, (b + 1) % bands) for b in range(first, bands, 2)]
        return lax.ppermute(mid, "band", ups + [(t, s) for s, t in ups])

    far, near = exchange(1), exchange(0)
    gathered = call(
        gather_kernel,
        shape((2 * rows, edges), BF16),
        [VMEM] * 4,
        8,
        2 * edges * nodes * rows * 2,
        (mid, src, from_hot, to_hot),
    )
    by_node = call(
        edge_kernel,
        shape((nodes, share), BF16),
        [VMEM] * 7,
        24,
        2 * edges * nodes * 7 * 256,
        (near, far, into_edge, src, from_hot, to_hot, gathered),
        [pltpu.VMEM((nodes, share), F32)],
    )
    return call(
        node_kernel,
        shape((nodes, share), BF16),
        [VMEM] * 7,
        12,
        2 * nodes * share * 6 * share,
        (by_node, partner(by_node), mid, direct, embed_weight, agg, last),
    )


def solution(mesh):
    return jax.shard_map(
        on_device,
        mesh=mesh,
        in_specs=(
            P(None, "band"),
            P("band"),
            P("band", None),
            P("band"),
            P("band", None, None, None),
            P(None, "ch"),
            P("band"),
            P("band"),
            P(None, None, "ch"),
            P("ch", None),
            P(None, None, "ch"),
            P("ch", None),
        ),
        out_specs=P("band", "ch"),
        check_vma=False,
    )
```

```python
import functools

import jax
import jax.numpy as jnp
from jax import lax
from jax.experimental import pallas as pl
from jax.experimental.pallas import tpu as pltpu
from jax.sharding import PartitionSpec as P

F32 = jnp.float32
BF16 = jnp.bfloat16
VMEM = pl.BlockSpec(memory_space=pltpu.VMEM)
HBM = pl.BlockSpec(memory_space=pltpu.HBM)
SMEM = pl.BlockSpec(memory_space=pltpu.SMEM)
NT = (((1,), (1,)), ((), ()))
TN = (((0,), (0,)), ((), ()))


def silu(v):
    return v * (0.5 * jnp.tanh(0.5 * v) + 0.5)


def pack_kernel(band_points_ref, points_ref, out_ref, rows_ref, limit_ref, limit_sem, sems):
    core = lax.axis_index("ch")
    channels, half = rows_ref.shape
    parts = sems.shape[0]
    width = half // parts
    limit_copy = pltpu.make_async_copy(band_points_ref, limit_ref, limit_sem)
    limit_copy.start()
    copies = []
    for i in range(parts):
        start = pl.multiple_of((1 - core) * half + i * width, width)
        copies.append(
            pltpu.make_async_copy(
                points_ref.at[:, pl.ds(start, width)],
                rows_ref.at[:, i * width : (i + 1) * width],
                sems.at[i],
            )
        )
        copies[-1].start()
    limit_copy.wait()
    limit = jnp.where(core == 0, limit_ref[0] - half, half)
    full = channels // 8
    last = channels - 8 * full
    for i in range(parts):
        copies[i].wait()
        at = i * width
        live = at + lax.broadcasted_iota(jnp.int32, (8, width), 1) < limit
        for t in range(full):
            x = rows_ref[8 * t : 8 * t + 8, at : at + width]
            out_ref[:, t * half + at : t * half + at + width] = jnp.where(live, x, jnp.zeros_like(x))
        x = rows_ref[8 * full :, at : at + width]
        x = jnp.where(live[:last], x, jnp.zeros_like(x))
        low = at % (half * last // 8)
        row = (at // (half * last // 8)) * last
        out_ref[row : row + last, full * half + low : full * half + low + width] = x


def own_kernel(
    ids_ref, count_ref, limit_ref, weight_ref, points_ref, out_ref,
):
    band, core = lax.axis_index("band"), lax.axis_index("ch")
    channels = points_ref.shape[0]
    kblocks, _, block_len = weight_ref.shape
    sub_count = points_ref.shape[1] // block_len
    out_ref[...] = jnp.zeros_like(out_ref)
    for k in range(kblocks):
        local = ids_ref[0, k] - band * sub_count
        mine = (local >= 0) & (local < sub_count) & (core == k % 2) & (k < count_ref[0])

        @pl.when(mine)
        def _():
            at = pl.multiple_of(local * block_len, block_len)
            x = points_ref[:, pl.ds(at, block_len)]
            column = at + lax.broadcasted_iota(jnp.int32, x.shape, 1)
            x = jnp.where(column < limit_ref[0], x, jnp.zeros_like(x))
            out_ref[:channels, :] += lax.dot_general(
                x, weight_ref[k], NT, preferred_element_type=F32
            )


def hots_kernel(src_ref, dst_ref, from_ref, to_ref):
    band = lax.axis_index("band")
    nodes, edges = from_ref.shape
    size = edges // 10
    node = lax.broadcasted_iota(jnp.int32, (nodes, size), 0).astype(F32).astype(BF16)
    one, zero = jnp.ones((), BF16), jnp.zeros((), BF16)
    for at in range(0, edges, size):
        src = src_ref[:, at : at + size] - (band - 1) * nodes
        src = src - (src // nodes) * nodes
        dst = dst_ref[:, at : at + size] - band * nodes
        from_ref[:, at : at + size] = jnp.where(node == src.astype(F32).astype(BF16), one, zero)
        to_ref[:, at : at + size] = jnp.where(node == dst.astype(F32).astype(BF16), one, zero)


def gather_kernel(mid_ref, src_ref, from_ref, to_ref, out_ref):
    band = lax.axis_index("band")
    rows, nodes = mid_ref.shape
    edges = src_ref.shape[1]
    size = edges // 2
    for at in range(0, edges, size):
        piece = (src_ref[:, at : at + size] - (band - 1) * nodes) // nodes
        got = jnp.dot(mid_ref[...], from_ref[:, at : at + size], preferred_element_type=F32)
        out_ref[:rows, at : at + size] = jnp.where(piece == 1, got, 0.0).astype(BF16)
        got = jnp.dot(mid_ref[...], to_ref[:, at : at + size], preferred_element_type=F32)
        out_ref[rows:, at : at + size] = got.astype(BF16)


def halo_kernel(channels, ids_ref, count_ref, weight_ref, points_ref, own_ref, out_ref, slots):
    band, core = lax.axis_index("band"), lax.axis_index("ch")
    kblocks, _, block_len = weight_ref.shape
    half = points_ref.shape[1] * 8 // channels
    blocks = half // block_len
    sub_count = 2 * blocks
    full = channels // 8
    last = channels - 8 * full
    found = jnp.int32(0)
    for k in range(kblocks):
        local = ids_ref[0, k] - band * sub_count
        low = (core == 0) & (local < 0)
        high = (core == 1) & (local >= sub_count)
        mine = (low | high) & (k < count_ref[0])
        block = jnp.where(low, local + blocks, local - sub_count)

        @pl.when(mine)
        def _():
            slots[0, found] = k
            slots[1, found] = jnp.clip(block, 0, blocks - 1)

        found = found + mine.astype(jnp.int32)
    out_ref[...] = own_ref[...]
    group = 4
    for first in range(0, kblocks, group):

        @pl.when(first < found)
        def _():
            total = None
            for j in range(first, first + group):
                used = j < found
                k = jnp.where(used, slots[0, j], 0)
                block = jnp.where(used, slots[1, j], 0)
                at = pl.multiple_of(block * block_len, block_len)
                x = [
                    points_ref[:, pl.ds(pl.multiple_of(t * half + at, block_len), block_len)]
                    for t in range(full)
                ]
                stack = half * last // 8
                low = pl.multiple_of(full * half + lax.rem(at, stack), block_len)
                tail = points_ref[:, pl.ds(low, block_len)].astype(F32)
                tail = jnp.where(at < stack, tail[:last], tail[last : 2 * last])
                x = jnp.concatenate([piece.astype(F32) for piece in x] + [tail], axis=0)
                x = jnp.where(used, x, 0.0).astype(BF16)
                part = lax.dot_general(x, weight_ref[k], NT, preferred_element_type=F32)
                total = part if total is None else total + part
            out_ref[:channels, :] += total


def weights_kernel(
    embed_ref, embed_other_ref, edge_in_ref, node_own_ref, node_other_ref,
    out_own_ref, out_other_ref, last_own_hbm, last_other_hbm,
    into_ref, direct_ref, agg_ref, last_ref, sems,
):
    core = lax.axis_index("ch")
    channels, share = embed_ref.shape
    own = pl.ds(pl.multiple_of(core * share, share), share)
    other = pl.ds(pl.multiple_of((1 - core) * share, share), share)

    copies = [
        pltpu.make_async_copy(half.at[:, own], last_ref.at[i], sems.at[i])
        for i, half in enumerate((last_own_hbm, last_other_hbm))
    ]
    for copy in copies:
        copy.start()

    def dot(a, b):
        return jnp.dot(a, b, preferred_element_type=F32)

    rows = direct_ref.shape[0]
    into_ref[...] = jnp.zeros_like(into_ref)
    direct_ref[...] = jnp.zeros_like(direct_ref)
    for i in range(2):
        v = dot(embed_ref[...], edge_in_ref[i, own, :])
        v += dot(embed_other_ref[...], edge_in_ref[i, other, :])
        into_ref[i * rows : i * rows + channels, :] = v.astype(BF16)
    for j, node_ref in enumerate((node_own_ref, node_other_ref)):
        columns = slice(j * share, (j + 1) * share)
        v = dot(embed_ref[...], node_ref[0, own, :])
        v += dot(embed_other_ref[...], node_ref[0, other, :])
        direct_ref[:channels, columns] = v.astype(BF16)
        for i, half_ref in enumerate((out_own_ref, out_other_ref)):
            agg_ref[i, :, columns] = dot(half_ref[...], node_ref[1]).astype(BF16)
    for copy in copies:
        copy.wait()


def edge_kernel(
    near_ref, far_ref, into_ref, src_ref, from_ref, to_ref, gathered_ref, out_ref, acc_ref
):
    band = lax.axis_index("band")
    rows, nodes = near_ref.shape
    edges = src_ref.shape[1]
    size = edges // 2
    even = lax.rem(band, 2) == 0
    low = jnp.where(even, far_ref[...], near_ref[...])
    high = jnp.where(even, near_ref[...], far_ref[...])
    sources = jnp.concatenate([low, high], axis=0)

    def before(at):
        piece = (src_ref[:, at : at + size] - (band - 1) * nodes) // nodes
        got = jnp.dot(sources, from_ref[:, at : at + size], preferred_element_type=F32)
        got = jnp.where(piece == 0, got[:rows], jnp.where(piece == 2, got[rows:], 0.0))
        from_src = got.astype(BF16) + gathered_ref[:rows, at : at + size]
        both = jnp.concatenate([from_src, gathered_ref[rows:, at : at + size]], axis=0)
        return lax.dot_general(into_ref[...], both, TN, preferred_element_type=F32)

    acc_ref[...] = jnp.zeros_like(acc_ref)
    now = before(0)
    for at in range(0, edges, size):
        later = before(at + size) if at + size < edges else None
        hidden = silu(now.astype(BF16))
        acc_ref[...] += lax.dot_general(
            to_ref[:, at : at + size], hidden, NT, preferred_element_type=F32
        )
        now = later
    out_ref[...] = acc_ref[...].astype(out_ref.dtype)


def node_kernel(own_ref, other_ref, mid_ref, direct_ref, embed_ref, agg_ref, last_ref, out_ref):
    channels, share = embed_ref.shape
    v = lax.dot_general(mid_ref[...], direct_ref[...], TN, preferred_element_type=F32)
    v += jnp.dot(own_ref[...], agg_ref[0], preferred_element_type=F32)
    v += jnp.dot(other_ref[...], agg_ref[1], preferred_element_type=F32)
    update = silu(v).astype(BF16)
    v = lax.dot_general(mid_ref[:channels, :], embed_ref[...], TN, preferred_element_type=F32)
    v += jnp.dot(update[:, :share], last_ref[0], preferred_element_type=F32)
    v += jnp.dot(update[:, share:], last_ref[1], preferred_element_type=F32)
    out_ref[...] = v.astype(out_ref.dtype)


def call(kernel, out, specs, limit_mib, flops, args, scratch=()):
    return pl.pallas_call(
        kernel,
        out_shape=out,
        in_specs=specs,
        out_specs=[VMEM] * len(out) if isinstance(out, tuple) else VMEM,
        scratch_shapes=list(scratch),
        compiler_params=pltpu.CompilerParams(vmem_limit_bytes=int(limit_mib * 2**20)),
        cost_estimate=pl.CostEstimate(flops=flops, bytes_accessed=1 << 20, transcendentals=0),
    )(*args)


def on_device(
    grid_field,
    band_points,
    block_ids,
    block_count,
    block_weight,
    embed_weight,
    edge_src,
    edge_dst,
    edge_in_weight,
    edge_out_weight,
    node_in_weight,
    node_out_weight,
):
    bands = lax.axis_size("band")
    channels, points = grid_field.shape
    _, kblocks, nodes, block_len = block_weight.shape
    share = embed_weight.shape[1]
    edges = edge_src.shape[0]
    half = points // 2
    rows = -(-channels // 16) * 16
    weight = block_weight[0]
    shape = jax.ShapeDtypeStruct

    pairs = [(2 * b, 2 * b + 2) for b in range(bands - 1)] + [(2 * bands - 2, 2 * bands - 1)]
    pairs += [(2 * b + 3, 2 * b + 1) for b in range(bands - 1)] + [(1, 0)]
    piece = call(
        pack_kernel,
        pltpu.VMEM((8, channels * half // 8), BF16),
        [HBM, HBM],
        61,
        1 << 20,
        (band_points, grid_field),
        [
            pltpu.VMEM((channels, half), BF16),
            pltpu.SMEM((1,), jnp.int32),
            pltpu.SemaphoreType.DMA,
            pltpu.SemaphoreType.DMA((8,)),
        ],
    )
    halo = lax.ppermute(piece, ("band", "ch"), pairs)

    def partner(x):
        return lax.ppermute(x, "ch", [(0, 1), (1, 0)])

    embed_other = partner(embed_weight)
    out_other = partner(edge_out_weight)
    node_other = partner(node_in_weight)
    last_other = partner(node_out_weight)
    src, dst = edge_src.reshape(1, edges), edge_dst.reshape(1, edges)
    remap_flops = 2 * channels * nodes * block_len * kblocks // 4
    sums = shape((rows, nodes), F32)
    partial = call(
        own_kernel,
        sums,
        [SMEM] * 3 + [VMEM] * 2,
        16,
        8 * remap_flops,
        (block_ids, block_count, band_points, weight, grid_field),
    )
    from_hot, to_hot = call(
        hots_kernel,
        (shape((nodes, edges), BF16), shape((nodes, edges), BF16)),
        [VMEM] * 2,
        4,
        edges * nodes * 16,
        (src, dst),
    )
    into_edge, direct, agg, last = call(
        weights_kernel,
        (
            shape((2 * rows, share), BF16),
            shape((rows, 2 * share), BF16),
            shape((2, share, 2 * share), BF16),
            shape((2, share, share), BF16),
        ),
        [VMEM] * 7 + [HBM] * 2,
        18,
        16 * share**3,
        (
            embed_weight,
            embed_other,
            edge_in_weight,
            node_in_weight,
            node_other,
            edge_out_weight,
            out_other,
            node_out_weight,
            last_other,
        ),
        [pltpu.SemaphoreType.DMA((2,))],
    )

    partial = call(
        functools.partial(halo_kernel, channels),
        sums,
        [SMEM] * 2 + [VMEM] * 3,
        12,
        remap_flops,
        (block_ids, block_count, weight, halo, partial),
        [pltpu.SMEM((2, kblocks), jnp.int32)],
    )
    mid = (partial + partner(partial)).astype(BF16)

    def exchange(first):
        ups = [(b, b + 1) for b in range(first, bands - 1, 2)]
        moves = [(2 * x + c, 2 * y + c) for b, t in ups for x, y in ((b, t), (t, b)) for c in (0, 1)]
        alone = set(range(bands)) - {b for up in ups for b in up}
        moves += [(2 * b + c, 2 * b + 1 - c) for b in sorted(alone) for c in (0, 1)]
        return lax.ppermute(mid, ("band", "ch"), moves)

    far, near = exchange(1), exchange(0)
    gathered = call(
        gather_kernel,
        shape((2 * rows, edges), BF16),
        [VMEM] * 4,
        8,
        2 * edges * nodes * rows * 2,
        (mid, src, from_hot, to_hot),
    )
    by_node = call(
        edge_kernel,
        shape((nodes, share), BF16),
        [VMEM] * 7,
        24,
        2 * edges * nodes * 7 * 256,
        (near, far, into_edge, src, from_hot, to_hot, gathered),
        [pltpu.VMEM((nodes, share), F32)],
    )
    return call(
        node_kernel,
        shape((nodes, share), BF16),
        [VMEM] * 7,
        12,
        2 * nodes * share * 6 * share,
        (by_node, partner(by_node), mid, direct, embed_weight, agg, last),
    )


def solution(mesh):
    return jax.shard_map(
        on_device,
        mesh=mesh,
        in_specs=(
            P(None, "band"),
            P("band"),
            P("band", None),
            P("band"),
            P("band", None, None, None),
            P(None, "ch"),
            P("band"),
            P("band"),
            P(None, None, "ch"),
            P("ch", None),
            P(None, None, "ch"),
            P("ch", None),
        ),
        out_specs=P("band", "ch"),
        check_vma=False,
    )
```

```python
import functools

import jax
import jax.numpy as jnp
from jax import lax
from jax.experimental import pallas as pl
from jax.experimental.pallas import tpu as pltpu
from jax.sharding import PartitionSpec as P

F32 = jnp.float32
BF16 = jnp.bfloat16
VMEM = pl.BlockSpec(memory_space=pltpu.VMEM)
HBM = pl.BlockSpec(memory_space=pltpu.HBM)
SMEM = pl.BlockSpec(memory_space=pltpu.SMEM)
NT = (((1,), (1,)), ((), ()))
TN = (((0,), (0,)), ((), ()))


def silu(v):
    return v * (0.5 * jnp.tanh(0.5 * v) + 0.5)


def pack_kernel(half, offset, band_points_ref, points_ref, out_ref, rows_ref, limit_ref, limit_sem, sems):
    core = lax.axis_index("ch")
    channels, run = rows_ref.shape
    parts = sems.shape[0]
    width = run // parts
    limit_copy = pltpu.make_async_copy(band_points_ref, limit_ref, limit_sem)
    limit_copy.start()
    copies = []
    for i in range(parts):
        start = pl.multiple_of((1 - core) * half + offset + i * width, width)
        copies.append(
            pltpu.make_async_copy(
                points_ref.at[:, pl.ds(start, width)],
                rows_ref.at[:, i * width : (i + 1) * width],
                sems.at[i],
            )
        )
        copies[-1].start()
    limit_copy.wait()
    limit = jnp.where(core == 0, limit_ref[0] - half, half) - offset
    full = channels // 8
    last = channels - 8 * full
    for i in range(parts):
        copies[i].wait()
        at = i * width
        live = at + lax.broadcasted_iota(jnp.int32, (8, width), 1) < limit
        for t in range(full):
            x = rows_ref[8 * t : 8 * t + 8, at : at + width]
            out_ref[:, t * run + at : t * run + at + width] = jnp.where(live, x, jnp.zeros_like(x))
        x = rows_ref[8 * full :, at : at + width]
        x = jnp.where(live[:last], x, jnp.zeros_like(x))
        low = at % (run * last // 8)
        row = (at // (run * last // 8)) * last
        out_ref[row : row + last, full * run + low : full * run + low + width] = x


def own_kernel(
    ids_ref, count_ref, limit_ref, weight_ref, points_ref, out_ref,
):
    band, core = lax.axis_index("band"), lax.axis_index("ch")
    channels = points_ref.shape[0]
    kblocks, _, block_len = weight_ref.shape
    sub_count = points_ref.shape[1] // block_len
    out_ref[...] = jnp.zeros_like(out_ref)
    for k in range(kblocks):
        local = ids_ref[0, k] - band * sub_count
        mine = (local >= 0) & (local < sub_count) & (core == k % 2) & (k < count_ref[0])

        @pl.when(mine)
        def _():
            at = pl.multiple_of(local * block_len, block_len)
            x = points_ref[:, pl.ds(at, block_len)]
            column = at + lax.broadcasted_iota(jnp.int32, x.shape, 1)
            x = jnp.where(column < limit_ref[0], x, jnp.zeros_like(x))
            out_ref[:channels, :] += lax.dot_general(
                x, weight_ref[k], NT, preferred_element_type=F32
            )


def hots_kernel(src_ref, dst_ref, from_ref, to_ref):
    band = lax.axis_index("band")
    nodes, edges = from_ref.shape
    size = edges // 10
    node = lax.broadcasted_iota(jnp.int32, (nodes, size), 0).astype(F32).astype(BF16)
    one, zero = jnp.ones((), BF16), jnp.zeros((), BF16)
    for at in range(0, edges, size):
        src = src_ref[:, at : at + size] - (band - 1) * nodes
        src = src - (src // nodes) * nodes
        dst = dst_ref[:, at : at + size] - band * nodes
        from_ref[:, at : at + size] = jnp.where(node == src.astype(F32).astype(BF16), one, zero)
        to_ref[:, at : at + size] = jnp.where(node == dst.astype(F32).astype(BF16), one, zero)


def gather_kernel(mid_ref, src_ref, from_ref, to_ref, out_ref):
    band = lax.axis_index("band")
    rows, nodes = mid_ref.shape
    edges = src_ref.shape[1]
    size = edges // 2
    for at in range(0, edges, size):
        piece = (src_ref[:, at : at + size] - (band - 1) * nodes) // nodes
        got = jnp.dot(mid_ref[...], from_ref[:, at : at + size], preferred_element_type=F32)
        out_ref[:rows, at : at + size] = jnp.where(piece == 1, got, 0.0).astype(BF16)
        got = jnp.dot(mid_ref[...], to_ref[:, at : at + size], preferred_element_type=F32)
        out_ref[rows:, at : at + size] = got.astype(BF16)


def halo_kernel(channels, ids_ref, count_ref, weight_ref, early_ref, late_ref, own_ref, out_ref, slots):
    band, core = lax.axis_index("band"), lax.axis_index("ch")
    kblocks, _, block_len = weight_ref.shape
    runs = [ref.shape[1] * 8 // channels for ref in (early_ref, late_ref)]
    blocks = sum(runs) // block_len
    sub_count = 2 * blocks
    full = channels // 8
    last = channels - 8 * full

    def rows_of(ref, run, at):
        x = [
            ref[:, pl.ds(pl.multiple_of(t * run + at, block_len), block_len)].astype(F32)
            for t in range(full)
        ]
        stack = run * last // 8
        low = pl.multiple_of(full * run + lax.rem(at, stack), block_len)
        tail = ref[:, pl.ds(low, block_len)].astype(F32)
        tail = jnp.where(at < stack, tail[:last], tail[last : 2 * last])
        return jnp.concatenate(x + [tail], axis=0)

    found = jnp.int32(0)
    for k in range(kblocks):
        local = ids_ref[0, k] - band * sub_count
        low = (core == 0) & (local < 0)
        high = (core == 1) & (local >= sub_count)
        mine = (low | high) & (k < count_ref[0])
        block = jnp.where(low, local + blocks, local - sub_count)

        @pl.when(mine)
        def _():
            slots[0, found] = k
            slots[1, found] = jnp.clip(block, 0, blocks - 1)

        found = found + mine.astype(jnp.int32)
    out_ref[...] = own_ref[...]
    group = 4
    for first in range(0, kblocks, group):

        @pl.when(first < found)
        def _():
            total = None
            for j in range(first, first + group):
                used = j < found
                k = jnp.where(used, slots[0, j], 0)
                block = jnp.where(used, slots[1, j], 0)
                at = pl.multiple_of(block * block_len, block_len)
                x = jnp.where(
                    at < runs[0],
                    rows_of(early_ref, runs[0], jnp.minimum(at, runs[0] - block_len)),
                    rows_of(late_ref, runs[1], jnp.maximum(at - runs[0], 0)),
                )
                x = jnp.where(used, x, 0.0).astype(BF16)
                part = lax.dot_general(x, weight_ref[k], NT, preferred_element_type=F32)
                total = part if total is None else total + part
            out_ref[:channels, :] += total


def weights_kernel(
    embed_ref, embed_other_ref, edge_in_ref, node_own_ref, node_other_ref,
    out_own_ref, out_other_ref, last_own_hbm, last_other_hbm,
    into_ref, direct_ref, agg_ref, last_ref, sems,
):
    core = lax.axis_index("ch")
    channels, share = embed_ref.shape
    own = pl.ds(pl.multiple_of(core * share, share), share)
    other = pl.ds(pl.multiple_of((1 - core) * share, share), share)

    copies = [
        pltpu.make_async_copy(half.at[:, own], last_ref.at[i], sems.at[i])
        for i, half in enumerate((last_own_hbm, last_other_hbm))
    ]
    for copy in copies:
        copy.start()

    def dot(a, b):
        return jnp.dot(a, b, preferred_element_type=F32)

    rows = direct_ref.shape[0]
    into_ref[...] = jnp.zeros_like(into_ref)
    direct_ref[...] = jnp.zeros_like(direct_ref)
    for i in range(2):
        v = dot(embed_ref[...], edge_in_ref[i, own, :])
        v += dot(embed_other_ref[...], edge_in_ref[i, other, :])
        into_ref[i * rows : i * rows + channels, :] = v.astype(BF16)
    for j, node_ref in enumerate((node_own_ref, node_other_ref)):
        columns = slice(j * share, (j + 1) * share)
        v = dot(embed_ref[...], node_ref[0, own, :])
        v += dot(embed_other_ref[...], node_ref[0, other, :])
        direct_ref[:channels, columns] = v.astype(BF16)
        for i, half_ref in enumerate((out_own_ref, out_other_ref)):
            agg_ref[i, :, columns] = dot(half_ref[...], node_ref[1]).astype(BF16)
    for copy in copies:
        copy.wait()


def edge_kernel(
    near_ref, far_ref, into_ref, src_ref, from_ref, to_ref, gathered_ref, out_ref, acc_ref
):
    band = lax.axis_index("band")
    rows, nodes = near_ref.shape
    edges = src_ref.shape[1]
    size = edges // 2
    even = lax.rem(band, 2) == 0
    low = jnp.where(even, far_ref[...], near_ref[...])
    high = jnp.where(even, near_ref[...], far_ref[...])
    sources = jnp.concatenate([low, high], axis=0)

    def before(at):
        piece = (src_ref[:, at : at + size] - (band - 1) * nodes) // nodes
        got = jnp.dot(sources, from_ref[:, at : at + size], preferred_element_type=F32)
        got = jnp.where(piece == 0, got[:rows], jnp.where(piece == 2, got[rows:], 0.0))
        from_src = got.astype(BF16) + gathered_ref[:rows, at : at + size]
        both = jnp.concatenate([from_src, gathered_ref[rows:, at : at + size]], axis=0)
        return lax.dot_general(into_ref[...], both, TN, preferred_element_type=F32)

    acc_ref[...] = jnp.zeros_like(acc_ref)
    now = before(0)
    for at in range(0, edges, size):
        later = before(at + size) if at + size < edges else None
        hidden = silu(now.astype(BF16))
        acc_ref[...] += lax.dot_general(
            to_ref[:, at : at + size], hidden, NT, preferred_element_type=F32
        )
        now = later
    out_ref[...] = acc_ref[...].astype(out_ref.dtype)


def node_kernel(own_ref, other_ref, mid_ref, direct_ref, embed_ref, agg_ref, last_ref, out_ref):
    channels, share = embed_ref.shape
    v = lax.dot_general(mid_ref[...], direct_ref[...], TN, preferred_element_type=F32)
    v += jnp.dot(own_ref[...], agg_ref[0], preferred_element_type=F32)
    v += jnp.dot(other_ref[...], agg_ref[1], preferred_element_type=F32)
    update = silu(v).astype(BF16)
    v = lax.dot_general(mid_ref[:channels, :], embed_ref[...], TN, preferred_element_type=F32)
    v += jnp.dot(update[:, :share], last_ref[0], preferred_element_type=F32)
    v += jnp.dot(update[:, share:], last_ref[1], preferred_element_type=F32)
    out_ref[...] = v.astype(out_ref.dtype)


def call(kernel, out, specs, limit_mib, flops, args, scratch=()):
    return pl.pallas_call(
        kernel,
        out_shape=out,
        in_specs=specs,
        out_specs=[VMEM] * len(out) if isinstance(out, tuple) else VMEM,
        scratch_shapes=list(scratch),
        compiler_params=pltpu.CompilerParams(vmem_limit_bytes=int(limit_mib * 2**20)),
        cost_estimate=pl.CostEstimate(flops=flops, bytes_accessed=1 << 20, transcendentals=0),
    )(*args)


def on_device(
    grid_field,
    band_points,
    block_ids,
    block_count,
    block_weight,
    embed_weight,
    edge_src,
    edge_dst,
    edge_in_weight,
    edge_out_weight,
    node_in_weight,
    node_out_weight,
):
    bands = lax.axis_size("band")
    channels, points = grid_field.shape
    _, kblocks, nodes, block_len = block_weight.shape
    share = embed_weight.shape[1]
    edges = edge_src.shape[0]
    half = points // 2
    rows = -(-channels // 16) * 16
    weight = block_weight[0]
    shape = jax.ShapeDtypeStruct

    pairs = [(2 * b, 2 * b + 2) for b in range(bands - 1)] + [(2 * bands - 2, 2 * bands - 1)]
    pairs += [(2 * b + 3, 2 * b + 1) for b in range(bands - 1)] + [(1, 0)]
    split = 6 * block_len

    def send(offset, run, limit):
        piece = call(
            functools.partial(pack_kernel, half, offset),
            pltpu.VMEM((8, channels * run // 8), BF16),
            [HBM, HBM],
            limit,
            1 << 20,
            (band_points, grid_field),
            [
                pltpu.VMEM((channels, run), BF16),
                pltpu.SMEM((1,), jnp.int32),
                pltpu.SemaphoreType.DMA,
                pltpu.SemaphoreType.DMA((run // block_len,)),
            ],
        )
        return lax.ppermute(piece, ("band", "ch"), pairs)

    early, late = send(0, split, 61), send(split, half - split, 40)

    def partner(x):
        return lax.ppermute(x, "ch", [(0, 1), (1, 0)])

    embed_other = partner(embed_weight)
    out_other = partner(edge_out_weight)
    node_other = partner(node_in_weight)
    last_other = partner(node_out_weight)
    src, dst = edge_src.reshape(1, edges), edge_dst.reshape(1, edges)
    remap_flops = 2 * channels * nodes * block_len * kblocks // 4
    sums = shape((rows, nodes), F32)
    partial = call(
        own_kernel,
        sums,
        [SMEM] * 3 + [VMEM] * 2,
        16,
        8 * remap_flops,
        (block_ids, block_count, band_points, weight, grid_field),
    )
    from_hot, to_hot = call(
        hots_kernel,
        (shape((nodes, edges), BF16), shape((nodes, edges), BF16)),
        [VMEM] * 2,
        4,
        edges * nodes * 16,
        (src, dst),
    )
    into_edge, direct, agg, last = call(
        weights_kernel,
        (
            shape((2 * rows, share), BF16),
            shape((rows, 2 * share), BF16),
            shape((2, share, 2 * share), BF16),
            shape((2, share, share), BF16),
        ),
        [VMEM] * 7 + [HBM] * 2,
        18,
        16 * share**3,
        (
            embed_weight,
            embed_other,
            edge_in_weight,
            node_in_weight,
            node_other,
            edge_out_weight,
            out_other,
            node_out_weight,
            last_other,
        ),
        [pltpu.SemaphoreType.DMA((2,))],
    )

    partial = call(
        functools.partial(halo_kernel, channels),
        sums,
        [SMEM] * 2 + [VMEM] * 4,
        12,
        remap_flops,
        (block_ids, block_count, weight, early, late, partial),
        [pltpu.SMEM((2, kblocks), jnp.int32)],
    )
    mid = (partial + partner(partial)).astype(BF16)

    def exchange(first):
        ups = [(b, b + 1) for b in range(first, bands - 1, 2)]
        moves = [(2 * x + c, 2 * y + c) for b, t in ups for x, y in ((b, t), (t, b)) for c in (0, 1)]
        alone = set(range(bands)) - {b for up in ups for b in up}
        moves += [(2 * b + c, 2 * b + 1 - c) for b in sorted(alone) for c in (0, 1)]
        return lax.ppermute(mid, ("band", "ch"), moves)

    far, near = exchange(1), exchange(0)
    gathered = call(
        gather_kernel,
        shape((2 * rows, edges), BF16),
        [VMEM] * 4,
        8,
        2 * edges * nodes * rows * 2,
        (mid, src, from_hot, to_hot),
    )
    by_node = call(
        edge_kernel,
        shape((nodes, share), BF16),
        [VMEM] * 7,
        24,
        2 * edges * nodes * 7 * 256,
        (near, far, into_edge, src, from_hot, to_hot, gathered),
        [pltpu.VMEM((nodes, share), F32)],
    )
    return call(
        node_kernel,
        shape((nodes, share), BF16),
        [VMEM] * 7,
        12,
        2 * nodes * share * 6 * share,
        (by_node, partner(by_node), mid, direct, embed_weight, agg, last),
    )


def solution(mesh):
    return jax.shard_map(
        on_device,
        mesh=mesh,
        in_specs=(
            P(None, "band"),
            P("band"),
            P("band", None),
            P("band"),
            P("band", None, None, None),
            P(None, "ch"),
            P("band"),
            P("band"),
            P(None, None, "ch"),
            P("ch", None),
            P(None, None, "ch"),
            P("ch", None),
        ),
        out_specs=P("band", "ch"),
        check_vma=False,
    )
```
